32 devices in a mesh: seq: 16 (over z, y, x), head: 2 (over core).
Axes of the slice: x: 2, y: 2, z: 4, core: 2. Of those that a mesh axis runs over, the one named last changes fastest.
Arguments:
- queries: bfloat16 [8192, 4096], P('seq', 'head'), may hold values from -80 to 80
- new_keys: bfloat16 [8192, 1024], P('seq', 'head'), may hold values from -8 to 8
- new_values: bfloat16 [8192, 1024], P('seq', 'head'), may hold values from -6 to 6
Outputs:
- attended: bfloat16 [8192, 4096], P('seq', 'head')
- key_low: float32 [64, 1024], P('seq', 'head')
- key_step: float32 [64, 1024], P('seq', 'head')
- value_low: float32 [8192], P('seq')
- value_step: float32 [8192], P('seq')
The draws below stay inside these ranges and needn't reach their ends.
All inputs are finite; a program needn't handle non-finite values.
Results may differ from the reference program's by a relative error of at most 0.0045.
Values may be sent and summed in bfloat16 or wider, within the bound.
A program may use at most 128 MiB of HBM per device.

```python
import math
import jax
import jax.numpy as jnp
from jax import lax

HEADS = 32
KV_HEADS = 8
HEAD_DIM = 128
WINDOW = 4096
GROUP = 128
TOK_DEV = 512
TOKENS = 8192


def draw_pair(base):
    width = KV_HEADS * HEAD_DIM
    key_rows = jnp.clip(jax.random.normal(jax.random.fold_in(base, 1), (TOKENS, width), jnp.float32), -6.0, 6.0)
    query_rows = 2.0 * jnp.clip(jax.random.normal(jax.random.fold_in(base, 2), (TOKENS, HEADS * HEAD_DIM), jnp.float32), -6.0, 6.0)
    return (query_rows, key_rows)


def draw_queries(key, part):
    query_rows, key_rows = draw_pair(jax.random.fold_in(key, 7))
    return query_rows.astype(jnp.bfloat16)


def draw_new_keys(key, part):
    query_rows, key_rows = draw_pair(jax.random.fold_in(key, 7))
    return key_rows.astype(jnp.bfloat16)


def shard_levels(rng, shape, cuts, low, largest):
    def one(axis_at, blocks):
        draws = jax.random.uniform(jax.random.fold_in(jax.random.fold_in(rng, 6), axis_at), (blocks,), jnp.float32, low / len(cuts), largest / len(cuts))
        return jnp.repeat(jnp.exp(draws), shape[axis_at] // blocks).reshape((-1,) + (1,) * (len(shape) - axis_at - 1))

    factor_of = one(*cuts[0])
    for cut in cuts[1:]:
        factor_of = factor_of * one(*cut)
    return factor_of


def scatter_about(key, extent, scale, most, cuts=(), kind=jnp.bfloat16):
    array = jax.random.normal(key, extent, jnp.float32) * scale
    if len(cuts) > 0:
        array = shard_levels(key, extent, cuts, -0.22, 0.18) * array
    return jnp.clip(array, min=-most, max=most).astype(kind)


def setup_inputs(seed: int = 0) -> dict:
    streams_of = jax.random.split(jax.random.key(seed), 4)
    return {
        "queries": draw_queries(jax.random.fold_in(streams_of[3], 71), 0),
        "new_keys": draw_new_keys(jax.random.fold_in(streams_of[3], 71), 0),
        "new_values": scatter_about(streams_of[2], (TOKENS, KV_HEADS * HEAD_DIM), 1.0, 6.0, ((0, 16), (1, 2))),
    }


negative_fill = -1e+30

def attend_head(inputs, valid, scale):
    query_head, key_head, value_head = inputs
    scores = jnp.einsum('qgd,kd->gqk', query_head.astype(jnp.float32), key_head.astype(jnp.float32), precision=lax.Precision.HIGHEST) * scale
    masked = jnp.where(valid[None], scores, negative_fill)
    peak = lax.optimization_barrier(jnp.max(masked, axis=-1, keepdims=True))
    weights = jnp.where(valid[None], jnp.exp(masked - peak), 0.0)
    total = lax.optimization_barrier(jnp.sum(weights, axis=-1, keepdims=True))
    rounded = lax.optimization_barrier(weights.astype(jnp.bfloat16)).astype(jnp.float32)
    numer = jnp.einsum('gqk,kd->gqd', rounded, value_head.astype(jnp.float32), precision=lax.Precision.HIGHEST)
    return (numer / total).astype(jnp.bfloat16)

def reference(queries, new_keys, new_values):
    group_size = HEADS // KV_HEADS
    scale = 1.0 / math.sqrt(HEAD_DIM)
    block = TOK_DEV
    nblocks = TOKENS // block
    span = WINDOW + block
    zeros_front = jnp.zeros((WINDOW, KV_HEADS * HEAD_DIM), jnp.bfloat16)
    key_padded = jnp.concatenate((zeros_front, new_keys), 0)
    value_padded = jnp.concatenate((zeros_front, new_values), 0)

    def per_block(index):
        start = (index * block).astype(jnp.int32)
        query_block = lax.dynamic_slice_in_dim(queries, start, block, 0).reshape(block, KV_HEADS, group_size, HEAD_DIM)
        key_window = lax.dynamic_slice_in_dim(key_padded, start, span, 0).reshape(span, KV_HEADS, HEAD_DIM)
        value_window = lax.dynamic_slice_in_dim(value_padded, start, span, 0).reshape(span, KV_HEADS, HEAD_DIM)
        query_pos = start + jnp.arange(block, dtype=jnp.int32)
        key_pos = start - WINDOW + jnp.arange(span, dtype=jnp.int32)
        valid = (key_pos[None, :] <= query_pos[:, None]) & (key_pos[None, :] > query_pos[:, None] - WINDOW) & (key_pos[None, :] >= 0)
        heads_out = lax.map(lambda inputs: attend_head(inputs, valid, scale), (jnp.transpose(query_block, (1, 0, 2, 3)), jnp.transpose(key_window, (1, 0, 2)), jnp.transpose(value_window, (1, 0, 2))))
        return jnp.transpose(heads_out, (2, 0, 1, 3)).reshape(block, HEADS * HEAD_DIM)
    attended = lax.map(per_block, jnp.arange(nblocks, dtype=jnp.int32)).reshape(TOKENS, HEADS * HEAD_DIM)
    grouped = new_keys.astype(jnp.float32).reshape(TOKENS // GROUP, GROUP, KV_HEADS * HEAD_DIM)
    key_low = lax.optimization_barrier(jnp.min(grouped, axis=1))
    key_step = (lax.optimization_barrier(jnp.max(grouped, axis=1)) - key_low) / 3.0
    value_rows = new_values.astype(jnp.float32)
    value_low = lax.optimization_barrier(jnp.min(value_rows, axis=1))
    value_step = (lax.optimization_barrier(jnp.max(value_rows, axis=1)) - value_low) / 3.0
    return (attended, key_low, key_step, value_low, value_step)
```

```python
import functools
import math

import jax
import jax.numpy as jnp
from jax import lax
from jax.experimental import pallas as pl
from jax.experimental.pallas import tpu as pltpu
from jax.sharding import PartitionSpec as P

HEADS = 32
KV_HEADS = 8
HEAD_DIM = 128
WINDOW = 4096
GROUP = 128

negative_fill = -1e30
query_tile = 256

OWN, FAR, NEAR, NEAR_A, NEAR_B, NEAR_C, MIX_A, MIX_B, MIX_C = range(9)


def attend_kernel(
    devices, layer, q_hbm, k_hbm, v_hbm, o_hbm, q_buf, o_buf, kv, acc, peak,
    q_sem, in_sem, out_sem, send_sem, recv_sem,
):
    rows = q_buf.shape[1]
    local = kv.shape[1]
    group = q_buf.shape[0] // local
    factor = math.log2(math.e) / math.sqrt(HEAD_DIM)
    me = lax.axis_index("seq")
    plane = me // layer
    place = lax.rem(me, layer)
    up = lax.rem(me + layer, devices)
    down = lax.rem(me + devices - layer, devices)
    bit_a = lax.rem(place, 2)
    bit_b = place // 2
    side_a = me + 1 - 2 * bit_a
    side_b = me + 2 - 4 * bit_b

    def q_copy(head, sub):
        col = pl.multiple_of((head * group + sub) * HEAD_DIM, HEAD_DIM)
        return pltpu.make_async_copy(
            q_hbm.at[:, pl.ds(col, HEAD_DIM)], q_buf.at[head * group + sub], q_sem.at[head, sub]
        )

    def out_copy(head, sub):
        col = pl.multiple_of((head * group + sub) * HEAD_DIM, HEAD_DIM)
        return pltpu.make_async_copy(
            o_buf.at[head * group + sub], o_hbm.at[:, pl.ds(col, HEAD_DIM)], out_sem.at[head, sub]
        )

    def own_copy(head, which):
        col = pl.multiple_of(head * HEAD_DIM, HEAD_DIM)
        source = (k_hbm, v_hbm)[which]
        return pltpu.make_async_copy(
            source.at[:, pl.ds(col, HEAD_DIM)], kv.at[OWN, head, which], in_sem.at[head, which]
        )

    def send(head, source, slot, target):
        return pltpu.make_async_remote_copy(
            src_ref=kv.at[source, head],
            dst_ref=kv.at[slot, head],
            send_sem=send_sem.at[slot, head],
            recv_sem=recv_sem.at[slot, head],
            device_id={"seq": target},
            device_id_type=pl.DeviceIdType.MESH,
        )

    routes = {
        NEAR: (OWN, up),
        FAR: (NEAR, up),
        NEAR_A: (NEAR, side_a),
        NEAR_B: (NEAR, side_b),
        NEAR_C: (NEAR_A, side_b),
        MIX_A: (bit_a, side_a),
        MIX_B: (bit_b, side_b),
        MIX_C: (MIX_B, side_a),
    }

    def transfer(head, slot):
        source, target = routes[slot]
        return send(head, source, slot, target)

    barrier = pltpu.get_barrier_semaphore()
    for other in (up, down, side_a, side_b):
        pl.semaphore_signal(
            barrier, inc=1, device_id={"seq": other}, device_id_type=pl.DeviceIdType.MESH
        )
    for head in range(local):
        for which in range(2):
            own_copy(head, which).start()
    for head in range(local):
        for sub in range(group):
            q_copy(head, sub).start()
    pl.semaphore_wait(barrier, 4)

    tiles = rows // query_tile

    def scores_of(q, slot, head):
        return lax.dot_general(
            q, kv[slot, head, 0], (((1,), (1,)), ((), ())), preferred_element_type=jnp.float32
        )

    def product_of(weights, slot, head):
        values = kv[slot, head, 1]
        wide = jnp.concatenate((values, jnp.ones_like(values)), 1)
        return jnp.dot(weights.astype(jnp.bfloat16), wide, preferred_element_type=jnp.float32)

    def step(head, slots, first=False):
        @pl.loop(0, group * tiles)
        def _(index):
            sub = index // tiles
            start = pl.multiple_of(lax.rem(index, tiles) * query_tile, query_tile)
            state = pl.ds(pl.multiple_of(index * query_tile, query_tile), query_tile)
            q = q_buf[head * group + sub, pl.ds(start, query_tile), :]
            scores = []
            for slot in slots:
                part = scores_of(q, slot, head)
                if slot == OWN:
                    row = start + lax.broadcasted_iota(jnp.int32, part.shape, 0)
                    column = lax.broadcasted_iota(jnp.int32, part.shape, 1)
                    near = column <= row
                    far = scores_of(q, FAR, head)
                    far = jnp.where(plane >= 2, far, negative_fill)
                    part = jnp.where(near, part, far)
                scores.append(part)
            top = functools.reduce(jnp.maximum, scores)
            top = jnp.max(top, axis=1, keepdims=True)
            if not first:
                before = peak[state, :]
                top = jnp.maximum(before, top)
                fade = jnp.exp2((before - top) * factor)
                peak[state, :] = top
            else:
                peak[state, :] = jnp.broadcast_to(top, (query_tile, HEAD_DIM))
            top = top[:, :1]
            total = None
            for slot, part in zip(slots, scores):
                weights = jnp.exp2((part - top) * factor)
                if slot == OWN:
                    product = product_of(jnp.where(near, weights, 0.0), OWN, head)
                    product += product_of(jnp.where(near, 0.0, weights), FAR, head)
                else:
                    product = product_of(weights, slot, head)
                total = product if total is None else total + product
            if first:
                acc[state, :] = total
            else:
                acc[state, :HEAD_DIM] = acc[state, :HEAD_DIM] * fade + total[:, :HEAD_DIM]
                acc[state, HEAD_DIM:] = acc[state, HEAD_DIM:] * fade + total[:, HEAD_DIM:]

    def steps(head, valid, all_valid, slots, first=False):
        @pl.when(all_valid)
        def _():
            step(head, slots, first)

        @pl.when(jnp.logical_not(all_valid))
        def _():
            for at, (slot, good) in enumerate(zip(slots, valid)):
                if good is None:
                    step(head, (slot,), first and at == 0)
                else:
                    pl.when(good)(functools.partial(step, head, (slot,)))

    def finish(head):
        for sub in range(group):
            spot = pl.ds(sub * rows, rows)
            o_buf[head * group + sub] = (
                acc[spot, :HEAD_DIM] / acc[spot, HEAD_DIM:]
            ).astype(o_buf.dtype)
            out_copy(head, sub).start()

    near_ok = plane >= 1
    far_ok = plane >= 2
    mix_a_ok = (plane >= 2) | (bit_a == 1)
    mix_b_ok = (plane >= 2) | (bit_b == 1)

    @pl.loop(0, local + 1)
    def _(now):
        last = now - 1

        @pl.when(now < local)
        def _():
            for which in range(2):
                own_copy(now, which).wait()
            transfer(now, NEAR).start()

        @pl.when(now >= 1)
        def _():
            transfer(last, MIX_B).wait_recv()
            transfer(last, MIX_A).wait_recv()
            transfer(last, MIX_C).start()
            transfer(last, NEAR_C).start()
            steps(last, (near_ok, mix_a_ok, mix_b_ok), far_ok, (NEAR_B, MIX_A, MIX_B))

        @pl.when(now < local)
        def _():
            transfer(now, NEAR).wait_recv()
            transfer(now, NEAR_A).start()
            transfer(now, NEAR_B).start()
            transfer(now, FAR).start()

        @pl.when(now >= 1)
        def _():
            transfer(last, MIX_C).wait_recv()
            transfer(last, NEAR_C).wait_recv()
            steps(last, (near_ok, mix_b_ok), far_ok, (NEAR_C, MIX_C))
            finish(last)

        @pl.when(now < local)
        def _():
            transfer(now, FAR).wait_recv()
            transfer(now, MIX_A).start()
            transfer(now, MIX_B).start()
            transfer(now, NEAR_A).wait_recv()
            transfer(now, NEAR_B).wait_recv()
            for sub in range(group):
                q_copy(now, sub).wait()
            steps(now, (None, near_ok, near_ok), near_ok, (OWN, NEAR, NEAR_A), True)

    @pl.loop(0, local)
    def _(head):
        for slot in routes:
            transfer(head, slot).wait_send()
        for sub in range(group):
            out_copy(head, sub).wait()


def attend(devices, queries, new_keys, new_values):
    rows, width = queries.shape
    local = new_keys.shape[1] // HEAD_DIM
    heads = width // HEAD_DIM
    group = heads // local
    halo = WINDOW // rows
    layer = halo // 2
    if layer != 4 or devices % layer or devices < 3 * layer:
        raise ValueError("window layout")
    kernel = functools.partial(attend_kernel, devices, layer)
    hbm = pl.BlockSpec(memory_space=pl.ANY)
    return pl.pallas_call(
        kernel,
        out_shape=jax.ShapeDtypeStruct(queries.shape, jnp.bfloat16),
        in_specs=[hbm] * 3,
        out_specs=hbm,
        scratch_shapes=[
            pltpu.VMEM((heads, rows, HEAD_DIM), jnp.bfloat16),
            pltpu.VMEM((heads, rows, HEAD_DIM), jnp.bfloat16),
            pltpu.VMEM((9, local, 2, rows, HEAD_DIM), jnp.bfloat16),
            pltpu.VMEM((group * rows, 2 * HEAD_DIM), jnp.float32),
            pltpu.VMEM((group * rows, HEAD_DIM), jnp.float32),
            pltpu.SemaphoreType.DMA((local, group)),
            pltpu.SemaphoreType.DMA((local, 2)),
            pltpu.SemaphoreType.DMA((local, group)),
            pltpu.SemaphoreType.DMA((9, local)),
            pltpu.SemaphoreType.DMA((9, local)),
        ],
        compiler_params=pltpu.CompilerParams(
            collective_id=0, has_side_effects=True, vmem_limit_bytes=60 * 1024 * 1024
        ),
        cost_estimate=pl.CostEstimate(
            flops=4 * rows * width * WINDOW,
            bytes_accessed=2 * 2 * rows * width,
            transcendentals=heads * rows * WINDOW,
        ),
    )(queries, new_keys, new_values)


def over_heads(values, devices, combine):
    distance = 1
    while distance < devices:
        route = [(i, i ^ distance) for i in range(devices)]
        values = combine(values, lax.ppermute(values, "head", route))
        distance *= 2
    return values


def shards(mesh_shape, queries, new_keys, new_values):
    tok_rows, kv_width = new_keys.shape
    value_rows = new_values.astype(jnp.float32)
    extremes = jnp.stack((jnp.max(value_rows, axis=1), -jnp.min(value_rows, axis=1)), 0)
    extremes = over_heads(extremes, mesh_shape["head"], jnp.maximum)
    row_bottom = -extremes[1]
    value_step_out = (extremes[0] - row_bottom) / 3.0
    grouped = new_keys.astype(jnp.float32).reshape(tok_rows // GROUP, GROUP, kv_width)
    key_low = jnp.min(grouped, axis=1)
    key_step_out = (jnp.max(grouped, axis=1) - key_low) / 3.0
    attended = attend(mesh_shape["seq"], queries, new_keys, new_values)
    return (attended, key_low, key_step_out, row_bottom, value_step_out)


def solution(mesh):
    return jax.shard_map(
        functools.partial(shards, dict(mesh.shape)),
        mesh=mesh,
        in_specs=(P("seq", "head"), P("seq", "head"), P("seq", "head")),
        out_specs=(P("seq", "head"), P("seq", "head"), P("seq", "head"), P("seq"), P("seq")),
        check_vma=False,
    )
```

```python
import functools
import math

import jax
import jax.numpy as jnp
from jax import lax
from jax.experimental import pallas as pl
from jax.experimental.pallas import tpu as pltpu
from jax.sharding import PartitionSpec as P

HEADS = 32
KV_HEADS = 8
HEAD_DIM = 128
WINDOW = 4096
GROUP = 128

negative_fill = -1e30
query_heads = 2

OWN, FAR, NEAR, NEAR_A, NEAR_B, NEAR_C, MIX_A, MIX_B, MIX_C = range(9)


def attend_kernel(
    devices, layer, q_hbm, k_hbm, v_hbm, o_hbm, q_buf, o_buf, kv, acc, peak,
    q_sem, in_sem, out_sem, send_sem, recv_sem,
):
    rows = o_buf.shape[1]
    local = kv.shape[1]
    group = o_buf.shape[0] // local
    query_tile = query_heads * rows
    factor = math.log2(math.e) / math.sqrt(HEAD_DIM)
    me = lax.axis_index("seq")
    plane = me // layer
    place = lax.rem(me, layer)
    up = lax.rem(me + layer, devices)
    down = lax.rem(me + devices - layer, devices)
    bit_a = lax.rem(place, 2)
    bit_b = place // 2
    side_a = me + 1 - 2 * bit_a
    side_b = me + 2 - 4 * bit_b

    def q_copy(head, sub):
        col = pl.multiple_of((head * group + sub) * HEAD_DIM, HEAD_DIM)
        return pltpu.make_async_copy(
            q_hbm.at[:, pl.ds(col, HEAD_DIM)], q_buf.at[head, pl.ds(sub * rows, rows)], q_sem.at[head, sub]
        )

    def out_copy(head, sub):
        col = pl.multiple_of((head * group + sub) * HEAD_DIM, HEAD_DIM)
        return pltpu.make_async_copy(
            o_buf.at[head * group + sub], o_hbm.at[:, pl.ds(col, HEAD_DIM)], out_sem.at[head, sub]
        )

    def own_copy(head, which):
        col = pl.multiple_of(head * HEAD_DIM, HEAD_DIM)
        source = (k_hbm, v_hbm)[which]
        return pltpu.make_async_copy(
            source.at[:, pl.ds(col, HEAD_DIM)], kv.at[OWN, head, which], in_sem.at[head, which]
        )

    def send(head, source, slot, target):
        return pltpu.make_async_remote_copy(
            src_ref=kv.at[source, head],
            dst_ref=kv.at[slot, head],
            send_sem=send_sem.at[slot, head],
            recv_sem=recv_sem.at[slot, head],
            device_id={"seq": target},
            device_id_type=pl.DeviceIdType.MESH,
        )

    routes = {
        NEAR: (OWN, up),
        FAR: (NEAR, up),
        NEAR_A: (NEAR, side_a),
        NEAR_B: (NEAR, side_b),
        NEAR_C: (NEAR_A, side_b),
        MIX_A: (bit_a, side_a),
        MIX_B: (bit_b, side_b),
        MIX_C: (MIX_B, side_a),
    }

    def transfer(head, slot):
        source, target = routes[slot]
        return send(head, source, slot, target)

    near_ok = plane >= 1
    far_ok = plane >= 2
    mix_a_ok = (plane >= 2) | (bit_a == 1)
    mix_b_ok = (plane >= 2) | (bit_b == 1)

    barrier = pltpu.get_barrier_semaphore()
    for other in (up, down, side_a, side_b):
        pl.semaphore_signal(
            barrier, inc=1, device_id={"seq": other}, device_id_type=pl.DeviceIdType.MESH
        )
    for head in range(local):
        for which in range(2):
            own_copy(head, which).start()
    for head in range(local):
        for sub in range(group):
            q_copy(head, sub).start()
    pl.semaphore_wait(barrier, 4)

    def lane_parts(block):
        return [block[:, at : at + HEAD_DIM] for at in range(0, block.shape[1], HEAD_DIM)]

    def scores_of(q, slot, head):
        return lax.dot_general(
            q, kv[slot, head, 0], (((1,), (1,)), ((), ())), preferred_element_type=jnp.float32
        )

    def product_of(weights, slot, head):
        product = jnp.dot(
            weights.astype(jnp.bfloat16), kv[slot, head, 1], preferred_element_type=jnp.float32
        )
        return product, functools.reduce(jnp.add, lane_parts(weights))

    def step(head, slots, valid, first=False):
        @pl.loop(0, group // query_heads)
        def _(index):
            state = pl.ds(pl.multiple_of(index * query_tile, query_tile), query_tile)
            q = q_buf[head, state, :]
            scores = []
            top = None
            for slot, good in zip(slots, valid):
                part = scores_of(q, slot, head)
                if slot == OWN:
                    square = (rows, part.shape[1])
                    row = lax.broadcasted_iota(jnp.int32, square, 0)
                    near = lax.broadcasted_iota(jnp.int32, square, 1) <= row
                    near = jnp.concatenate([near] * query_heads, 0) if query_heads > 1 else near
                    far = scores_of(q, FAR, head)
                    far = jnp.where(far_ok, far, negative_fill)
                    part = jnp.where(near, part, far)
                scores.append(part)
                peaks = functools.reduce(jnp.maximum, lane_parts(part))
                if good is not None:
                    peaks = jnp.where(good, peaks, negative_fill)
                top = peaks if top is None else jnp.maximum(top, peaks)
            top = jnp.max(top, axis=1, keepdims=True)
            if not first:
                before = peak[state, :]
                top = jnp.maximum(before, top)
                fade = jnp.exp2((before - top) * factor)
                peak[state, :] = top
            else:
                peak[state, :] = jnp.broadcast_to(top, (query_tile, HEAD_DIM))
            top = top[:, :1]
            pieces = []
            for slot, part, good in zip(slots, scores, valid):
                base = top if good is None else jnp.where(good, top, -negative_fill)
                weights = jnp.exp2((part - base) * factor)
                if slot == OWN:
                    pieces.append(product_of(jnp.where(near, weights, 0.0), OWN, head))
                    pieces.append(product_of(jnp.where(near, 0.0, weights), FAR, head))
                else:
                    pieces.append(product_of(weights, slot, head))
            product, lanes = (functools.reduce(jnp.add, each) for each in zip(*pieces))
            if not first:
                product += acc[state, :HEAD_DIM] * fade
                lanes += acc[state, HEAD_DIM:] * fade
            acc[state, :HEAD_DIM] = product
            acc[state, HEAD_DIM:] = lanes

    def finish(head):
        for sub in range(group):
            spot = pl.ds(sub * rows, rows)
            o_buf[head * group + sub] = (
                acc[spot, :HEAD_DIM] / jnp.sum(acc[spot, HEAD_DIM:], axis=1, keepdims=True)
            ).astype(o_buf.dtype)
            out_copy(head, sub).start()

    @pl.loop(0, local + 1)
    def _(now):
        last = now - 1

        @pl.when(now < local)
        def _():
            for which in range(2):
                own_copy(now, which).wait()
            transfer(now, NEAR).start()

        @pl.when(now >= 1)
        def _():
            transfer(last, MIX_B).wait_recv()
            transfer(last, MIX_A).wait_recv()
            transfer(last, MIX_C).start()
            transfer(last, NEAR_C).start()
            step(last, (NEAR_B, MIX_A, MIX_B), (near_ok, mix_a_ok, mix_b_ok))

        @pl.when(now < local)
        def _():
            transfer(now, NEAR).wait_recv()
            transfer(now, NEAR_A).start()
            transfer(now, NEAR_B).start()
            transfer(now, FAR).start()

        @pl.when(now >= 1)
        def _():
            transfer(last, MIX_C).wait_recv()
            transfer(last, NEAR_C).wait_recv()
            step(last, (NEAR_C, MIX_C), (near_ok, mix_b_ok))
            finish(last)

        @pl.when(now < local)
        def _():
            transfer(now, FAR).wait_recv()
            transfer(now, MIX_A).start()
            transfer(now, MIX_B).start()
            transfer(now, NEAR_A).wait_recv()
            transfer(now, NEAR_B).wait_recv()
            for sub in range(group):
                q_copy(now, sub).wait()
            step(now, (OWN, NEAR, NEAR_A), (None, near_ok, near_ok), True)

    @pl.loop(0, local)
    def _(head):
        for slot in routes:
            transfer(head, slot).wait_send()
        for sub in range(group):
            out_copy(head, sub).wait()


def attend(devices, queries, new_keys, new_values):
    rows, width = queries.shape
    local = new_keys.shape[1] // HEAD_DIM
    heads = width // HEAD_DIM
    group = heads // local
    halo = WINDOW // rows
    layer = halo // 2
    if layer != 4 or devices % layer or devices < 3 * layer:
        raise ValueError("window layout")
    kernel = functools.partial(attend_kernel, devices, layer)
    hbm = pl.BlockSpec(memory_space=pl.ANY)
    return pl.pallas_call(
        kernel,
        out_shape=jax.ShapeDtypeStruct(queries.shape, jnp.bfloat16),
        in_specs=[hbm] * 3,
        out_specs=hbm,
        scratch_shapes=[
            pltpu.VMEM((local, group * rows, HEAD_DIM), jnp.bfloat16),
            pltpu.VMEM((heads, rows, HEAD_DIM), jnp.bfloat16),
            pltpu.VMEM((9, local, 2, rows, HEAD_DIM), jnp.bfloat16),
            pltpu.VMEM((group * rows, 2 * HEAD_DIM), jnp.float32),
            pltpu.VMEM((group * rows, HEAD_DIM), jnp.float32),
            pltpu.SemaphoreType.DMA((local, group)),
            pltpu.SemaphoreType.DMA((local, 2)),
            pltpu.SemaphoreType.DMA((local, group)),
            pltpu.SemaphoreType.DMA((9, local)),
            pltpu.SemaphoreType.DMA((9, local)),
        ],
        compiler_params=pltpu.CompilerParams(
            collective_id=0, has_side_effects=True, vmem_limit_bytes=60 * 1024 * 1024
        ),
        cost_estimate=pl.CostEstimate(
            flops=4 * rows * width * WINDOW,
            bytes_accessed=2 * 2 * rows * width,
            transcendentals=heads * rows * WINDOW,
        ),
    )(queries, new_keys, new_values)


def over_heads(values, devices, combine):
    distance = 1
    while distance < devices:
        route = [(i, i ^ distance) for i in range(devices)]
        values = combine(values, lax.ppermute(values, "head", route))
        distance *= 2
    return values


def shards(mesh_shape, queries, new_keys, new_values):
    tok_rows, kv_width = new_keys.shape
    value_rows = new_values.astype(jnp.float32)
    extremes = jnp.stack((jnp.max(value_rows, axis=1), -jnp.min(value_rows, axis=1)), 0)
    extremes = over_heads(extremes, mesh_shape["head"], jnp.maximum)
    row_bottom = -extremes[1]
    value_step_out = (extremes[0] - row_bottom) / 3.0
    grouped = new_keys.astype(jnp.float32).reshape(tok_rows // GROUP, GROUP, kv_width)
    key_low = jnp.min(grouped, axis=1)
    key_step_out = (jnp.max(grouped, axis=1) - key_low) / 3.0
    attended = attend(mesh_shape["seq"], queries, new_keys, new_values)
    return (attended, key_low, key_step_out, row_bottom, value_step_out)


def solution(mesh):
    return jax.shard_map(
        functools.partial(shards, dict(mesh.shape)),
        mesh=mesh,
        in_specs=(P("seq", "head"), P("seq", "head"), P("seq", "head")),
        out_specs=(P("seq", "head"), P("seq", "head"), P("seq", "head"), P("seq"), P("seq")),
        check_vma=False,
    )
```
